256 devices in a mesh: atom: 4 (over y), pix: 64 (over z, x, core).
Axes of the slice: x: 4, y: 4, z: 8, core: 2. Of those that a mesh axis runs over, the one named last changes fastest.
Arguments:
- observed: float32 [224, 16384], P('atom', 'pix'), may hold values from -6 to 6
- library: float32 [224, 4096], P(None, ('atom', 'pix')), may hold values from -0.09375 to 0.09375
- image_split: float32 [224, 16384], P('atom', 'pix'), may hold values from -6 to 6
- image_dual: float32 [224, 16384], P('atom', 'pix'), may hold values from -4 to 4
- support: float32 [4096, 16384], P('atom', 'pix'), may hold values from -12 to 12
- support_dual: float32 [4096, 16384], P('atom', 'pix'), may hold values from -4 to 4
- positive: float32 [4096, 16384], P('atom', 'pix'), may hold values from 0 to 1
- positive_dual: float32 [4096, 16384], P('atom', 'pix'), may hold values from -4 to 4
Outputs:
- abundance: float32 [4096, 16384], P('atom', 'pix')
- image_split_next: float32 [224, 16384], P('atom', 'pix')
- image_dual_next: float32 [224, 16384], P('atom', 'pix')
- support_next: float32 [4096, 16384], P('atom', 'pix')
- support_dual_next: float32 [4096, 16384], P('atom', 'pix')
- positive_next: float32 [4096, 16384], P('atom', 'pix')
- positive_dual_next: float32 [4096, 16384], P('atom', 'pix')
The draws below stay inside these ranges and needn't reach their ends.
All inputs are finite; a program needn't handle non-finite values.
Results may differ from the reference program's by a relative error of at most 0.0001.
Values sent between devices are 32-bit elements; how exact they have to be, the bound alone decides.
A program may use at most 64 MiB of HBM per device.

```python
import math
import jax
import jax.numpy as jnp
from jax import lax

BANDS = 224
ATOMS = 4096
ITERS = 4
NPIX = 16384


def draw_support(key, part):
    first_key, second_key = jax.random.split(jax.random.fold_in(key, 11))
    scales = jnp.exp(jax.random.uniform(first_key, (ATOMS, 1), jnp.float32, math.log(0.05), math.log(3.0)))
    base = jnp.clip(jax.random.normal(second_key, (ATOMS, NPIX), jnp.float32), -4.0, 4.0)
    return (scales * base).astype(jnp.float32)


def steps_of(own_key, extent, pieces, least, top_value):
    def one(position, parts):
        steps = jax.random.uniform(jax.random.fold_in(jax.random.fold_in(own_key, 6), position), (parts,), jnp.float32, least / len(pieces), top_value / len(pieces))
        return jnp.repeat(jnp.exp(steps), extent[position] // parts).reshape((-1,) + (1,) * (len(extent) - position - 1))

    factor_of = one(*pieces[0])
    for cut in pieces[1:]:
        factor_of = factor_of * one(*cut)
    return factor_of


def bell_draw(stream_key, extent, deviation, bound, pieces=(), kind=jnp.bfloat16):
    factor_of = steps_of(stream_key, extent, pieces, -0.22, 0.18) if pieces else 1.0
    array = jax.random.normal(stream_key, extent, jnp.float32) * deviation * factor_of
    return jnp.minimum(jnp.maximum(array, -bound), bound).astype(kind)


def setup_inputs(seed: int = 0) -> dict:
    splits = jax.random.split(jax.random.key(seed), 9)
    return {
        "observed": bell_draw(splits[0], (BANDS, NPIX), 1.0, 6.0, ((0, 4), (1, 64)), jnp.float32),
        "library": bell_draw(splits[1], (BANDS, ATOMS), ATOMS ** -0.5, 0.09375, ((1, 256),), jnp.float32),
        "image_split": bell_draw(splits[2], (BANDS, NPIX), 1.0, 6.0, ((0, 4), (1, 64)), jnp.float32),
        "image_dual": bell_draw(splits[3], (BANDS, NPIX), 0.3, 4.0, ((0, 4), (1, 64)), jnp.float32),
        "support": draw_support(jax.random.fold_in(splits[8], 71), 0),
        "support_dual": bell_draw(splits[5], (ATOMS, NPIX), 0.3, 4.0, ((0, 4), (1, 64)), jnp.float32),
        "positive": jnp.clip(1.0 * jax.random.uniform(splits[6], (ATOMS, NPIX), jnp.float32) ** steps_of(splits[6], (ATOMS, NPIX), ((0, 4), (1, 64)), -0.2, 0.2), 0.0, 1.0),
        "positive_dual": bell_draw(splits[7], (ATOMS, NPIX), 0.3, 4.0, ((0, 4), (1, 64)), jnp.float32),
    }


penalty = 0.5
shrink_rate = 0.4
epsilon = 1e-06

def matmul(left, right):
    return jnp.dot(left.astype(jnp.float32), right.astype(jnp.float32), precision=lax.Precision.HIGHEST, preferred_element_type=jnp.float32)

def reference(observed, library, image_split, image_dual, support, support_dual, positive, positive_dual):
    identity = jnp.eye(BANDS, dtype=jnp.float32)
    gram = matmul(library, library.T)
    inverse = jnp.linalg.solve(gram + 2.0 * identity, identity)
    level = shrink_rate * math.sqrt(NPIX)
    abundance = support
    for step in range(ITERS):
        right = matmul(library.T, image_split + image_dual) + support + support_dual + positive + positive_dual
        solved = matmul(inverse, matmul(library, right))
        abundance = 0.5 * (right - matmul(library.T, solved))
        mixed = matmul(library, abundance)
        image_split = (observed + penalty * (mixed - image_dual)) / (1.0 + penalty)
        image_dual = image_dual - (mixed - image_split)
        spread = abundance - support_dual
        squares = lax.optimization_barrier(jnp.sum(spread * spread, axis=1))
        support = spread * jnp.maximum(1.0 - level / jnp.sqrt(squares + epsilon), 0.0)[:, None]
        support_dual = support_dual - (abundance - support)
        positive = jnp.maximum(abundance - positive_dual, 0.0)
        positive_dual = positive_dual - (abundance - positive)
    return (abundance, image_split, image_dual, support, support_dual, positive, positive_dual)
```

```python
import functools
import math

import jax
import jax.numpy as jnp
from jax import lax
from jax.experimental import pallas as pl
from jax.experimental.pallas import tpu as pltpu
from jax.sharding import PartitionSpec as P

ITERS = 4
PENALTY = 0.5
SHRINK = 0.4
EPS = 1e-06
NX, NC = 4, 2
LEAF = 32
MESH = pl.DeviceIdType.MESH
HIGHEST = lax.Precision.HIGHEST
F32 = jnp.float32
BF16 = jnp.bfloat16
Z_ORDER = (1, 7, 2, 6, 3, 5, 4)
A_ORDER = (2, 1, 3)


def dot(left, right, precision=None):
    return jnp.dot(left, right, precision=precision, preferred_element_type=F32)


def halves(value):
    high = value.astype(BF16)
    return high, (value - high.astype(F32)).astype(BF16)


def remote(src, dst, send, recv, device):
    return pltpu.make_async_remote_copy(
        src_ref=src,
        dst_ref=dst,
        send_sem=send,
        recv_sem=recv,
        device_id=device,
        device_id_type=MESH,
    )


def kernel(
    level,
    obs_h, lib_h, split_h, dual_h, sup_h, sd_h, pos_h, pd_h,
    a_o, split_o, dual_o, sup_o, sd_o, pos_o, pd_o,
    w, spr, tt, w_hi, w_lo, lt, ltn, lmat, lrot, l_hi, l_lo, b_hi, b_lo,
    gram_mine, gram_in, full, own_inv, y_out, y_in, r_buf, obs, c_now,
    csend, z_in, psend, p_in,
    local_sem,
    gz_s, gz_r, gx_s, gx_r, gc_s, gc_r, gm_s, gm_r, gs_s, gs_r,
    y_s, y_r, r_s, r_r, z_s, z_r, p_s, p_r,
):
    n_atom = lax.axis_size("atom")
    n_pix = lax.axis_size("pix")
    nz = n_pix // (NX * NC)
    me = lax.axis_index("atom")
    pix = lax.axis_index("pix")
    z, x, c = pix // (NX * NC), (pix // NC) % NX, pix % NC
    bands = 224
    own = bands // n_atom
    atoms, pixels = w.shape
    shard = atoms // n_pix
    lane = lax.broadcasted_iota(jnp.int32, (8, 128), 1)

    def at(a, zz, xx, cc):
        return (a, zz * (NX * NC) + xx * NC + cc)

    def atom_peer(d):
        return ((me + d) % n_atom, pix)

    def z_peer(d):
        return at(me, (z + d) % nz, x, c)

    def plane_peer(e):
        dx, dc = e // NC, e % NC
        return at(me, z, (x + dx) % NX, (c + dc) % NC)

    loads = [
        pltpu.make_async_copy(src, dst, local_sem.at[i])
        for i, (src, dst) in enumerate(
            ((sup_h, spr), (sd_h, sd_o), (pos_h, tt), (pd_h, pd_o), (obs_h, obs), (split_h, split_o), (dual_h, dual_o))
        )
    ]
    slot = pl.multiple_of(((c * NX + x) * nz + z) * shard, shard)
    mine = pltpu.make_async_copy(lib_h, lt.at[pl.ds(slot, shard)], local_sem.at[7])
    mine.start()
    for copy in loads:
        copy.start()

    barrier = pltpu.get_barrier_semaphore()
    peers = [atom_peer(d) for d in range(1, 4)] + [z_peer(d) for d in range(1, 8)] + [plane_peer(e) for e in range(1, 8)]
    for peer in peers:
        pl.semaphore_signal(barrier, inc=1, device_id=peer, device_id_type=MESH)
    pl.semaphore_wait(barrier, len(peers))
    mine.wait()

    def rows_of(cc, xx, zz):
        return pl.ds(pl.multiple_of(((cc * NX + xx) * nz + zz) * shard, shard), shard)

    z_copies = {}
    for d in Z_ORDER:
        own_rows = rows_of(c, x, z)
        z_copies[d] = remote(lt.at[own_rows], lt.at[own_rows], gz_s.at[d - 1], gz_r.at[d - 1], z_peer(d))
        z_copies[d].start()
    x_copies = {}
    for d in (0,) + Z_ORDER:
        if d:
            z_copies[d].wait_recv()
        rows = rows_of(c, x, (z - d + nz) % nz)
        for dx in (2, 1, 3):
            x_copies[d, dx] = remote(
                lt.at[rows], lt.at[rows], gx_s.at[dx - 1, d], gx_r.at[dx - 1, d], at(me, z, (x + dx) % NX, c)
            )
            x_copies[d, dx].start()

    for i in range(4):
        loads[i].wait()

    def first(i, _):
        rows = pl.ds(pl.multiple_of(i * 16, 16), 16)
        value = ((spr[rows, :] + sd_o[rows, :]) + tt[rows, :]) + pd_o[rows, :]
        w[rows, :] = value
        high, low = halves(value)
        w_hi[rows, :] = high
        w_lo[rows, :] = low
        return 0

    lax.fori_loop(0, atoms // 16, first, 0, unroll=4)
    for i in range(ITERS):
        r_buf[i, bands:, :] = jnp.zeros((r_buf.shape[1] - bands, pixels), F32)

    half = NX * nz * shard
    group = nz * shard
    c_copies = []
    for dx in (0, 1, 3, 2):
        if dx:
            for d in (0,) + Z_ORDER:
                x_copies[d, dx].wait_recv()
        rows = pl.ds(pl.multiple_of(c * half + ((x - dx + NX) % NX) * group, group), group)
        copy = remote(lt.at[rows], lt.at[rows], gc_s.at[dx], gc_r.at[dx], at(me, z, x, (c + 1) % NC))
        copy.start()
        c_copies.append(copy)
    for copy in c_copies:
        copy.wait_recv()

    def arrange(p, _):
        zz, xx, cc = p // (NX * NC), (p // NC) % NX, p % NC
        ltn[pl.ds(pl.multiple_of(p * shard, shard), shard), :] = lt[rows_of(cc, xx, zz), :]
        return 0

    lax.fori_loop(0, n_pix, arrange, 0, unroll=4)
    lmat[...] = ltn[...].T

    gram = dot(lmat[...], ltn[...], HIGHEST)
    gram_mine[...] = gram
    part = 128
    half_rows = pl.ds(pl.multiple_of(c * part, part), part)
    g_copies = []
    for i, d in enumerate(A_ORDER):
        copy = remote(gram_mine.at[half_rows], gram_in.at[i], gm_s.at[i], gm_r.at[i], atom_peer(d))
        copy.start()
        g_copies.append(copy)

    for i, d in enumerate(A_ORDER + (0,)):
        rows = pl.ds(pl.multiple_of(((me + d) % n_atom) * own, own), own)
        lrot[i * own:(i + 1) * own, :] = lmat[rows, :]
    high, low = halves(lrot[...])
    l_hi[...] = high
    l_lo[...] = low

    def y_copy(k, i, d):
        return remote(y_out.at[pl.ds(i * own, own)], y_in.at[k, i], y_s.at[k, i], y_r.at[k, i], atom_peer(d))

    own_rows_r = pl.ds(pl.multiple_of(me * own, own), own)

    def r_copy(k, i, d):
        return remote(r_buf.at[k, own_rows_r], r_buf.at[k, own_rows_r], r_s.at[k, i], r_r.at[k, i], atom_peer(d))

    def head(k):
        high, low = w_hi[...], w_lo[...]
        y_out[...] = (dot(l_hi[...], low) + dot(l_lo[...], high)) + dot(l_hi[...], high)
        for i, d in enumerate(A_ORDER):
            y_copy(k, i, d).start()

    def middle(k):
        for i, d in enumerate(A_ORDER):
            y_copy(k, i, d).wait_recv()
        total = (y_out[3 * own:, :] + y_in[k, 0]) + (y_in[k, 1] + y_in[k, 2])
        r_buf[k, own_rows_r, :] = 2.0 * c_now[...] - total
        for i, d in enumerate(A_ORDER):
            r_copy(k, i, d).start()
        for i, d in enumerate(A_ORDER):
            y_copy(k, i, d).wait_send()

    def z_copy(k, d):
        return remote(csend.at[k], z_in.at[k, d - 1], z_s.at[k, d - 1], z_r.at[k, d - 1], z_peer(d))

    def p_copy(k, e):
        return remote(psend.at[k], p_in.at[k, e - 1], p_s.at[k, e - 1], p_r.at[k, e - 1], plane_peer(e))

    def tail(k):
        for i, d in enumerate(A_ORDER):
            r_copy(k, i, d).wait_recv()
        r_hi, r_lo = halves(r_buf[k])
        for ch in range(atoms // 256):
            rows = pl.ds(ch * 256, 256)
            spr[rows, :] = (dot(b_hi[rows, :], r_lo) + dot(b_lo[rows, :], r_hi)) + dot(b_hi[rows, :], r_hi)

        def rowwise(i, acc):
            rows = pl.ds(pl.multiple_of(i * 8, 8), 8)
            a = 0.5 * w[rows, :] + spr[rows, :]
            a_o[rows, :] = a
            spread = a - sd_o[rows, :]
            spr[rows, :] = spread
            tt[rows, :] = a - pd_o[rows, :]
            square = jnp.sum(spread * spread, axis=1, keepdims=True)
            return jnp.where(lane == i, square, acc)

        csend[k] = lax.fori_loop(0, atoms // 8, rowwise, jnp.zeros((8, 128), F32), unroll=8)
        for d in Z_ORDER[::-1]:
            z_copy(k, d).start()
        u = dot(own_inv[...], r_buf[k], HIGHEST)
        mixed = c_now[...] - u
        dual = dual_o[...]
        split = (obs[...] + PENALTY * (mixed - dual)) / (1.0 + PENALTY)
        dual = dual - (mixed - split)
        split_o[...] = split
        dual_o[...] = dual
        c_now[...] = split + dual
        for d in Z_ORDER:
            z_copy(k, d).wait_recv()
        total = csend[k]
        for d in range(1, 8):
            total = total + z_in[k, d - 1]
        psend[k] = total
        for e in range(7, 0, -1):
            p_copy(k, e).start()
        for i, d in enumerate(A_ORDER):
            r_copy(k, i, d).wait_send()
        for d in Z_ORDER:
            z_copy(k, d).wait_send()
        for e in range(1, 8):
            p_copy(k, e).wait_recv()
        total = psend[k]
        for e in range(1, 8):
            total = total + p_in[k, e - 1]
        for e in range(1, 8):
            p_copy(k, e).wait_send()
        return jnp.maximum(1.0 - level / jnp.sqrt(total + EPS), 0.0)

    def factor_of(factor, i):
        return jnp.sum(jnp.where(lane == i, factor, 0.0), axis=1, keepdims=True)

    def follow(factor):
        def rowwise(i, _):
            rows = pl.ds(pl.multiple_of(i * 16, 16), 16)
            f = jnp.concatenate([factor_of(factor, 2 * i), factor_of(factor, 2 * i + 1)], axis=0)
            spread, t = spr[rows, :], tt[rows, :]
            value = (2.0 * f - 1.0) * spread + jnp.abs(t)
            sd_o[rows, :] = (f - 1.0) * spread
            pd_o[rows, :] = jnp.maximum(-t, 0.0)
            w[rows, :] = value
            high, low = halves(value)
            w_hi[rows, :] = high
            w_lo[rows, :] = low
            return 0

        lax.fori_loop(0, atoms // 16, rowwise, 0, unroll=4)

    def finish(factor):
        def rowwise(i, _):
            rows = pl.ds(pl.multiple_of(i * 8, 8), 8)
            f = factor_of(factor, i)
            spread, t = spr[rows, :], tt[rows, :]
            sup_o[rows, :] = f * spread
            sd_o[rows, :] = (f - 1.0) * spread
            pos_o[rows, :] = jnp.maximum(t, 0.0)
            pd_o[rows, :] = jnp.maximum(-t, 0.0)
            return 0

        lax.fori_loop(0, atoms // 8, rowwise, 0, unroll=8)

    head(0)
    for i in range(4, 7):
        loads[i].wait()
    c_now[...] = split_o[...] + dual_o[...]

    for copy in g_copies:
        copy.wait_recv()
    size = full.shape[0]
    row = lax.broadcasted_iota(jnp.int32, (size, size), 0)
    col = lax.broadcasted_iota(jnp.int32, (size, size), 1)
    full[half_rows, :] = (gram_mine[half_rows, :] + gram_in[0]) + (gram_in[1] + gram_in[2])
    swap = remote(full.at[half_rows], full.at[half_rows], gs_s, gs_r, at(me, z, x, (c + 1) % NC))
    swap.start()
    middle(0)
    swap.wait_recv()
    swap.wait_send()
    full[...] = full[...] + jnp.where(row == col, 2.0, 0.0)

    panel_row = lax.broadcasted_iota(jnp.int32, (LEAF, size), 0)
    panel_col = lax.broadcasted_iota(jnp.int32, (LEAF, size), 1)

    def sweep(_, carry):
        panel = full[0:LEAF, :]
        for k in range(0, LEAF, 2):
            col1, col2 = panel[:, k:k + 1], panel[:, k + 1:k + 2]
            row1, row2 = panel[k:k + 1, :], panel[k + 1:k + 2, :]
            p11 = panel[k:k + 1, k:k + 1]
            p12 = panel[k:k + 1, k + 1:k + 2]
            p22 = panel[k + 1:k + 2, k + 1:k + 2]
            inv_det = 1.0 / (p11 * p22 - p12 * p12)
            i11, i12, i22 = p22 * inv_det, -p12 * inv_det, p11 * inv_det
            pick = panel_col[0:1, :]
            m1 = jnp.where(pick == k, -i11, jnp.where(pick == k + 1, -i12, i11 * row1 + i12 * row2))
            m2 = jnp.where(pick == k, -i12, jnp.where(pick == k + 1, -i22, i12 * row1 + i22 * row2))
            kept = jnp.where((panel_col == k) | (panel_col == k + 1), 0.0, panel)
            rest = kept - col1 * m1 - col2 * m2
            panel = jnp.where(panel_row == k, m1, jnp.where(panel_row == k + 1, m2, rest))
        now = full[...]
        change = dot(now[:, 0:LEAF], panel, HIGHEST)
        rest = jnp.where(col < LEAF, 0.0, now) - change
        new = jnp.concatenate([rest[LEAF:, :], panel], axis=0)
        full[...] = pltpu.roll(new, size - LEAF, 1)
        return carry

    lax.fori_loop(0, bands // LEAF, sweep, 0)
    now = full[...]
    now = jnp.concatenate([now[LEAF:, :], now[0:LEAF, :]], axis=0)
    full[...] = -pltpu.roll(now, size - LEAF, 1)
    own_inv[...] = full[own_rows_r, :]
    for ch in range(atoms // 256):
        rows = pl.ds(ch * 256, 256)
        high, low = halves(0.5 * dot(ltn[rows, :], full[...], HIGHEST))
        b_hi[rows, :] = high
        b_lo[rows, :] = low

    for copy in list(z_copies.values()) + list(x_copies.values()) + c_copies + g_copies:
        copy.wait_send()

    def step(k, carry):
        factor = tail(k)
        follow(factor)
        head(k + 1)
        middle(k + 1)
        return carry

    lax.fori_loop(0, ITERS - 1, step, 0)
    finish(tail(ITERS - 1))


def on_device(observed, library, image_split, image_dual, support, support_dual, positive, positive_dual):
    own, pixels = observed.shape
    bands = library.shape[0]
    atoms = support.shape[0]
    n_atom, n_pix = lax.axis_size("atom"), lax.axis_size("pix")
    nz = n_pix // (NX * NC)
    size = 256
    level = SHRINK * math.sqrt(n_pix * pixels)
    shard_t = jnp.pad(library.T, ((0, 0), (0, size - bands)))
    big = jax.ShapeDtypeStruct((atoms, pixels), F32)
    image = jax.ShapeDtypeStruct((own, pixels), F32)
    dma = pltpu.SemaphoreType.DMA
    vmem = pltpu.VMEM
    return pl.pallas_call(
        functools.partial(kernel, level),
        out_shape=(big, image, image, big, big, big, big),
        in_specs=[pl.BlockSpec(memory_space=pl.ANY)] * 8,
        out_specs=[pl.BlockSpec(memory_space=pltpu.VMEM)] * 7,
        scratch_shapes=[
            vmem((atoms, pixels), F32), vmem((atoms, pixels), F32), vmem((atoms, pixels), F32),
            vmem((atoms, pixels), BF16), vmem((atoms, pixels), BF16),
            vmem((atoms, size), F32), vmem((atoms, size), F32), vmem((size, atoms), F32),
            vmem((bands, atoms), F32), vmem((bands, atoms), BF16), vmem((bands, atoms), BF16),
            vmem((atoms, size), BF16), vmem((atoms, size), BF16),
            vmem((size, size), F32), vmem((3, size // 2, size), F32), vmem((size, size), F32),
            vmem((own, size), F32),
            vmem((bands, pixels), F32), vmem((ITERS, 3, own, pixels), F32), vmem((ITERS, size, pixels), F32),
            vmem((own, pixels), F32), vmem((own, pixels), F32),
            vmem((ITERS, 8, 128), F32), vmem((ITERS, 7, 8, 128), F32),
            vmem((ITERS, 8, 128), F32), vmem((ITERS, 7, 8, 128), F32),
            dma((8,)),
            dma((7,)), dma((7,)), dma((3, 8)), dma((3, 8)), dma((4,)), dma((4,)),
            dma((3,)), dma((3,)), dma, dma,
            dma((ITERS, 3)), dma((ITERS, 3)), dma((ITERS, 3)), dma((ITERS, 3)),
            dma((ITERS, 7)), dma((ITERS, 7)), dma((ITERS, 7)), dma((ITERS, 7)),
        ],
        compiler_params=pltpu.CompilerParams(
            collective_id=0, has_side_effects=True, vmem_limit_bytes=60 * 1024 * 1024
        ),
    )(observed, shard_t, image_split, image_dual, support, support_dual, positive, positive_dual)


def solution(mesh):
    split = P("atom", "pix")
    return jax.shard_map(
        on_device,
        mesh=mesh,
        in_specs=(split, P(None, ("atom", "pix"))) + (split,) * 6,
        out_specs=(split,) * 7,
        check_vma=False,
    )
```
